256 devices in a mesh: section: 2 (over y_hi), dp: 16 (over z, core), vocab: 8 (over y_lo, x).
Axes of the slice: x: 4, y: 4 (y_hi: 2, y_lo: 2; y = y_hi * 2 + y_lo), z: 8, core: 2. Of those that a mesh axis runs over, the one named last changes fastest.
Arguments:
- activations: bfloat16 [2, 2048, 2048], P('section', 'dp'), may hold values from -32 to 32
- token_ids: int32 [2, 2048], replicated, may hold values from 0 to 65535
- embed_table: bfloat16 [65536, 2048], P(('dp', 'vocab')), may hold values from -3 to 3
Outputs:
- tied_grad: bfloat16 [128, 2, 256, 2048], P(('dp', 'vocab'), 'section')
The draws below stay inside these ranges and needn't reach their ends.
All inputs are finite; a program needn't handle non-finite values.
Results may differ from the reference program's by a relative error of at most 0.0029.
Values may be sent and summed in bfloat16 or wider, within the bound.
A program may use at most 128 MiB of HBM per device.

```python
import math
import jax
import jax.numpy as jnp
import numpy as np
from jax import lax

D = 2048
VOCAB_DEV = 512
TOKENS = 2048
VOCAB = 65536
N_SECTION = 2


def table_rows(key, row_numbers):
    base_key = jax.random.fold_in(key, 101)

    def one_row(row_index):
        values = jax.random.normal(jax.random.fold_in(base_key, row_index), (D,), jnp.float32)
        return jnp.clip(values * (4.0 / math.sqrt(D)), -3.0, 3.0)
    return jax.vmap(one_row)(row_numbers)


def draw_embed_table(key, part):
    return table_rows(key, jnp.arange(VOCAB, dtype=jnp.int32)).astype(jnp.bfloat16)


def draw_activations(key, part):
    draw_key = jax.random.fold_in(key, 202)
    values = jax.random.normal(draw_key, (N_SECTION, TOKENS, D), jnp.float32)
    return jnp.clip(values, -32.0, 32.0).astype(jnp.bfloat16)


def plant(entries, stream_key, smallest, largest):
    spot = [jax.random.randint(jax.random.fold_in(stream_key, axis), (), 0, length) for axis, length in enumerate(entries.shape)]
    widest = entries.shape.index(max(entries.shape))
    beside = spot[:widest] + [(spot[widest] + 1) % entries.shape[widest]] + spot[widest + 1:]
    return entries.at[tuple(spot)].set(smallest).at[tuple(beside)].set(largest)


def rank_table(number_of, lean):
    portions = [(1 << 20) // math.isqrt(standing ** lean) + 1 for standing in range(1, number_of + 1)]
    scale = 1 + sum(portions) // (1 << 30)
    return np.cumsum(np.array([max(1, weight // scale) for weight in portions]))


def ranked(stream_key, shape, count, slope):
    listing = rank_table(count, slope)
    pick = jax.random.randint(jax.random.fold_in(stream_key, 1), shape, 0, int(listing[count - 1]))
    grade = jnp.searchsorted(jnp.asarray(listing, jnp.int32), pick, side="right")
    return jax.random.permutation(jax.random.fold_in(stream_key, 2), count)[grade].astype(jnp.int32)


def setup_inputs(seed: int = 0) -> dict:
    arg_keys = jax.random.split(jax.random.key(seed), 4)
    return {
        "activations": draw_activations(jax.random.fold_in(arg_keys[3], 71), 0),
        "token_ids": plant(ranked(arg_keys[1], (N_SECTION, TOKENS), VOCAB, 1), jax.random.fold_in(arg_keys[1], 3), 0, VOCAB - 1).astype(jnp.int32),
        "embed_table": draw_embed_table(jax.random.fold_in(arg_keys[3], 71), 0),
    }


def reference(activations, token_ids, embed_table):
    cotangent = activations[0]
    hidden = activations[1]
    input_ids = token_ids[0]
    target_ids = token_ids[1]
    blocks = embed_table.shape[0] // VOCAB_DEV
    table_blocks = embed_table.reshape(blocks, VOCAB_DEV, D)
    offsets = jnp.arange(blocks, dtype=jnp.int32) * VOCAB_DEV
    columns = jnp.arange(VOCAB_DEV, dtype=jnp.int32)

    def scores(table_slab):
        return jnp.dot(hidden, table_slab.T, preferred_element_type=jnp.float32)

    def running(state_pair, table_slab):
        row_peak, row_total = state_pair
        logits = scores(table_slab)
        new_peak = jnp.maximum(row_peak, jnp.max(logits, axis=1))
        row_total = row_total * jnp.exp(row_peak - new_peak) + jnp.sum(jnp.exp(logits - new_peak[:, None]), axis=1)
        return (new_peak, row_total), None

    initial = (jnp.full((TOKENS,), -1e30, jnp.float32), jnp.zeros((TOKENS,), jnp.float32))
    (row_peak, row_total), _ = lax.scan(running, initial, table_blocks)

    def block_gradient(block_pair):
        table_slab, offset = block_pair
        logits = scores(table_slab)
        target_hot = (target_ids[:, None] == offset + columns[None, :]).astype(jnp.float32)
        input_hot = (input_ids[:, None] == offset + columns[None, :]).astype(jnp.bfloat16)
        last_section = (jnp.exp(logits - row_peak[:, None]) / row_total[:, None] - target_hot).astype(jnp.bfloat16)
        gradient = jnp.dot(last_section.T, hidden, preferred_element_type=jnp.float32)
        gradient = gradient + jnp.dot(input_hot.T, cotangent, preferred_element_type=jnp.float32)
        return gradient.astype(jnp.bfloat16)

    gradients = lax.map(block_gradient, (table_blocks, offsets))
    return gradients.reshape(blocks, N_SECTION, VOCAB_DEV // N_SECTION, D)
```

```python
import jax
import jax.numpy as jnp
from jax import lax
from jax.experimental import pallas as pl
from jax.experimental.pallas import tpu as pltpu
from jax.sharding import PartitionSpec as P

MESH = pl.DeviceIdType.MESH
COT, HID = 0, 1
Z, X, Y = 8, 4, 4
SLOTS = ((0, 1), (1, 2), (3, 2), (5, 2), (7, 1))
WIDTH = 2048
CUT_X, CUT_Y = 1024, 1664
COLUMNS = ((0, CUT_X), (CUT_X, CUT_Y - CUT_X), (CUT_Y, WIDTH - CUT_Y))
ROWS = 256
DOT = dict(preferred_element_type=jnp.float32)


def merge(pairs):
    peak = pairs[0][0]
    for other, _ in pairs[1:]:
        peak = jnp.maximum(peak, other)
    total = pairs[0][1] * jnp.exp(pairs[0][0] - peak)
    for other, part in pairs[1:]:
        total = total + part * jnp.exp(other - peak)
    return peak, total


def kernel(
    act, ids, table, out,
    buf, tab, scores, last_w, first_w, acc, out_v,
    own_stat, core_stat, sent_stat, x_stat, y_stat, z_stat, fin_stat,
    local_sem, boot_s, boot_r, z_s, z_r, ring_s, ring_r, core_s, core_r, stat_s, stat_r,
):
    s = lax.axis_index("section")
    d = lax.axis_index("dp")
    v = lax.axis_index("vocab")
    z, c = lax.div(d, 2), lax.rem(d, 2)
    yl, x = lax.div(v, 4), lax.rem(v, 4)
    y = 2 * s + yl
    row_first = (d * 8 + v) * 512 + s * ROWS

    def z_dev(k):
        return {"dp": lax.rem(z + k + Z, Z) * 2 + c}

    def x_dev(k):
        return {"vocab": yl * 4 + lax.rem(x + k + X, X)}

    def y_dev(k):
        to = lax.rem(y + k + Y, Y)
        return {"section": lax.div(to, 2), "vocab": lax.rem(to, 2) * 4 + x}

    core_dev = {"dp": z * 2 + 1 - c}
    cross_dev = {"section": 1 - s, "vocab": (1 - yl) * 4 + x}

    def remote(src, dst, send, recv, device):
        return pltpu.make_async_remote_copy(
            src_ref=src, dst_ref=dst, send_sem=send, recv_sem=recv,
            device_id=device, device_id_type=MESH,
        )

    load_own = pltpu.make_async_copy(act, buf.at[s, 0, c], local_sem.at[0])
    load_own.start()
    load_table = pltpu.make_async_copy(table.at[pl.ds(s * ROWS, ROWS)], tab, local_sem.at[1])
    load_table.start()

    barrier = pltpu.get_barrier_semaphore()
    peers = [z_dev(k) for k in range(1, Z)] + [x_dev(k) for k in range(1, X)]
    peers += [y_dev(k) for k in range(1, Y)] + [core_dev]
    for peer in peers:
        pl.semaphore_signal(barrier, inc=1, device_id=peer, device_id_type=MESH)

    def region(array, slot, count, part, tile, tiles):
        first, width = COLUMNS[part]
        return buf.at[array, pl.ds(slot, count), c, pl.ds(tile, tiles), :, pl.ds(first, width)]

    def boot_copy(k):
        far_y = 3 - y
        if k == 0:
            ref = region(s, 0, 1, 0, 2 * x, 2)
        elif k == 1:
            ref = region(s, 0, 1, 1, 2 * far_y, 2)
        elif k == 2:
            ref = region(s, 0, 1, 2, 0, 8)
        elif k < 6:
            ref = region(s, 0, 1, 0, 2 * lax.rem(x + k - 2, X), 2)
        else:
            ref = region(s, 0, 1, 1, 2 * lax.rem(far_y + k - 5, Y), 2)
        return remote(ref, ref, boot_s.at[k], boot_r.at[k], cross_dev)

    def z_copy(array, way, t, part):
        slot = 0 if t == 0 else 2 * t - 1 + way
        to = 2 * t + 1 + way if t < 3 else 7
        quarter = 2 * (x, y, 0)[part]
        tiles = (2, 2, 8)[part]
        if t == 3:
            tiles = tiles // 2
            quarter = quarter + way * tiles
        return remote(
            region(array, slot, 1, part, quarter, tiles),
            region(array, to, 1, part, quarter, tiles),
            z_s.at[array, way, t, part], z_r.at[array, way, t, part],
            z_dev(1 if way == 0 else -1),
        )

    def ring_copy(array, dim, t, k):
        slot, count = SLOTS[t]
        q, dev = ((x, x_dev), (y, y_dev))[dim]
        if k < 2:
            tile, tiles = 2 * q, 2
        elif k == 2:
            tile, tiles = 2 * lax.rem(q + 3, 4), 1
        else:
            tile, tiles = 2 * lax.rem(q + 1, 4) + 1, 1
        ref = region(array, slot, count, dim, tile, tiles)
        return remote(
            ref, ref, ring_s.at[array, dim, t - 1, k], ring_r.at[array, dim, t - 1, k],
            dev(1 if k % 2 == 0 else -1),
        )

    def core_copy(array, t):
        slot, count = SLOTS[t]
        ref = buf.at[array, pl.ds(slot, count), c]
        return remote(ref, ref, core_s.at[array, t], core_r.at[array, t], core_dev)

    def start(array):
        for part in range(3):
            @pl.when(s != array)
            def _():
                boot_copy(part).wait_recv()

            for way in range(2):
                z_copy(array, way, 0, part).start()

    def step_quarters(array, t):
        for part in range(2):
            for way in range(2):
                z_copy(array, way, t - 1, part).wait_recv()
                if t < 4:
                    z_copy(array, way, t, part).start()
            for k in range(2):
                ring_copy(array, part, t, k).start()

    def step_whole(array, t):
        for way in range(2):
            z_copy(array, way, t - 1, 2).wait_recv()
            if t < 4:
                z_copy(array, way, t, 2).start()

    def pass_on(array, t):
        for dim in range(2):
            for k in range(2):
                ring_copy(array, dim, t, k).wait_recv()
                ring_copy(array, dim, t, k + 2).start()

    def share(array, t):
        for dim in range(2):
            for k in range(2):
                ring_copy(array, dim, t, k + 2).wait_recv()
        core_copy(array, t).start()

    def chip_of(slot):
        half = lax.div(slot + 1, 2)
        return lax.rem(z + jnp.where(lax.rem(slot, 2) == 1, Z - half, half), Z)

    def score(t):
        core_copy(HID, t).wait_recv()
        first, count = SLOTS[t]

        def one(slot, carry):
            rows = buf[HID, slot].reshape(256, WIDTH)
            block = lax.dot_general(tab[...], rows, (((1,), (1,)), ((), ())), **DOT)
            scores[slot] = block
            peak = jnp.max(block, axis=0, keepdims=True)
            total = jnp.sum(jnp.exp(block - peak), axis=0, keepdims=True)
            chip = chip_of(slot)
            for core in range(2):
                lanes = slice(core * 128, core * 128 + 128)
                own_stat[core, 0, pl.ds(chip, 1), :] = peak[:, lanes]
                own_stat[core, 1, pl.ds(chip, 1), :] = total[:, lanes]
            return carry

        lax.fori_loop(first, first + count, one, 0)

    def add_first(first, count, finish):
        def one(n, carry):
            cols = pl.ds(pl.multiple_of(n * 256, 256), 256)
            rows = buf[COT, pl.ds(first, count), :, :, :, cols].reshape(count * 256, 256)
            part = jnp.dot(first_w[:, first * 256 : (first + count) * 256], rows, **DOT)
            total = acc[:, cols] + part
            if finish:
                out_v[:, cols] = total.astype(jnp.bfloat16)
                pltpu.make_async_copy(
                    out_v.at[:, cols], out.at[:, cols], local_sem.at[2 + n]
                ).start()
            else:
                acc[:, cols] = total
            return carry

        lax.fori_loop(0, WIDTH // 256, one, 0)

    def hot(index, slot, core):
        at = pl.multiple_of(chip_of(slot) * 256 + core * 128, 128)
        wanted = ids[pl.ds(index, 1), pl.ds(at, 128)] - row_first
        return lax.broadcasted_iota(jnp.int32, (ROWS, 128), 0) == wanted

    def lanes_of(slot, core):
        return pl.ds(pl.multiple_of(slot * 256 + core * 128, 128), 128)

    def stat_core(k):
        if k == 0:
            return remote(own_stat.at[1 - c], core_stat, stat_s.at[0], stat_r.at[0], core_dev)
        return remote(sent_stat.at[3], fin_stat.at[c], stat_s.at[1], stat_r.at[1], core_dev)

    def stat_axis(axis, k):
        into, dev, at = ((x_stat, x_dev, 2), (y_stat, y_dev, 5), (z_stat, z_dev, 8))[axis]
        at = at + k - 1
        return remote(sent_stat.at[axis], into.at[k - 1], stat_s.at[at], stat_r.at[at], dev(k))

    counts = (X, Y, Z)

    def stat_send(axis, pairs):
        peak, total = merge(pairs)
        sent_stat[axis, 0] = peak
        sent_stat[axis, 1] = total
        if axis < 3:
            for k in range(1, counts[axis]):
                stat_axis(axis, k).start()

    def stat_take(axis):
        into = (x_stat, y_stat, z_stat)[axis]
        pairs = [(sent_stat[axis, 0], sent_stat[axis, 1])]
        for k in range(1, counts[axis]):
            stat_axis(axis, k).wait_recv()
            pairs.append((into[k - 1, 0], into[k - 1, 1]))
        return pairs

    load_own.wait()
    pl.semaphore_wait(barrier, len(peers))

    for k in range(3):
        boot_copy(k).start()
    start(HID)
    for k in range(3, 9):
        boot_copy(k).start()

    @pl.when(s == HID)
    def _():
        core_copy(HID, 0).start()

    @pl.when(s == COT)
    def _():
        core_copy(COT, 0).start()

    def first_rows(slot, carry):
        for core in range(2):
            first_w[:, lanes_of(slot, core)] = hot(0, slot, core).astype(jnp.bfloat16)
        return carry

    lax.fori_loop(0, 8, first_rows, 0)
    load_table.wait()

    step_quarters(HID, 1)
    step_whole(HID, 1)

    @pl.when(s == COT)
    def _():
        for k in range(3, 9):
            boot_copy(k).wait_recv()
        core_copy(HID, 0).start()

    step_quarters(HID, 2)
    pass_on(HID, 1)
    step_whole(HID, 2)
    step_quarters(HID, 3)
    pass_on(HID, 2)
    step_whole(HID, 3)
    share(HID, 1)
    score(0)
    start(COT)

    @pl.when(s == HID)
    def _():
        for k in range(3, 9):
            boot_copy(k).wait_recv()
        core_copy(COT, 0).start()

    step_quarters(HID, 4)
    pass_on(HID, 3)
    step_whole(HID, 4)
    share(HID, 2)
    score(1)
    pass_on(HID, 4)
    share(HID, 3)
    score(2)
    step_quarters(COT, 1)
    step_whole(COT, 1)
    share(HID, 4)
    score(3)
    score(4)
    stat_core(0).start()
    step_quarters(COT, 2)
    pass_on(COT, 1)
    stat_core(0).wait_recv()
    mine = own_stat[pl.ds(c, 1)]
    stat_send(0, [(mine[0, 0], mine[0, 1]), (core_stat[0], core_stat[1])])
    step_whole(COT, 2)
    stat_send(1, stat_take(0))
    step_quarters(COT, 3)
    pass_on(COT, 2)
    stat_send(2, stat_take(1))
    step_whole(COT, 3)
    share(COT, 1)
    stat_send(3, stat_take(2))
    stat_core(1).start()
    fin_stat[pl.ds(c, 1)] = sent_stat[pl.ds(3, 1)]
    step_quarters(COT, 4)
    pass_on(COT, 3)
    step_whole(COT, 4)
    share(COT, 2)
    pass_on(COT, 4)
    stat_core(1).wait_recv()

    def last_rows(slot, carry):
        chip = chip_of(slot)
        for core in range(2):
            peak = fin_stat[core, 0, pl.ds(chip, 1), :]
            total = fin_stat[core, 1, pl.ds(chip, 1), :]
            lanes = slice(core * 128, core * 128 + 128)
            probs = jnp.exp(scores[slot, :, lanes] - peak) / total
            weight = probs - jnp.where(hot(1, slot, core), 1.0, 0.0)
            last_w[:, lanes_of(slot, core)] = weight.astype(jnp.bfloat16)
        return carry

    lax.fori_loop(0, 8, last_rows, 0)

    def last_dot(n, carry):
        cols = pl.ds(pl.multiple_of(n * 256, 256), 256)
        rows = buf[HID, :, :, :, :, cols].reshape(2048, 256)
        acc[:, cols] = jnp.dot(last_w[...], rows, **DOT)
        return carry

    lax.fori_loop(0, WIDTH // 256, last_dot, 0)
    share(COT, 3)
    for t in range(3):
        core_copy(COT, t).wait_recv()
    add_first(0, 5, False)
    share(COT, 4)
    for t in range(3, 5):
        core_copy(COT, t).wait_recv()
    add_first(5, 3, True)

    for k in range(9):
        boot_copy(k).wait_send()
    for array in range(2):
        for part in range(3):
            for way in range(2):
                for t in range(4):
                    z_copy(array, way, t, part).wait_send()
        for t in range(1, 5):
            for dim in range(2):
                for k in range(4):
                    ring_copy(array, dim, t, k).wait_send()
        for t in range(5):
            core_copy(array, t).wait_send()
    for k in range(2):
        stat_core(k).wait_send()
    for axis in range(3):
        for k in range(1, counts[axis]):
            stat_axis(axis, k).wait_send()
    for n in range(WIDTH // 256):
        cols = pl.ds(n * 256, 256)
        pltpu.make_async_copy(out_v.at[:, cols], out.at[:, cols], local_sem.at[2 + n]).wait()


def body(activations, token_ids, embed_table):
    bf16, f32, dma = jnp.bfloat16, jnp.float32, pltpu.SemaphoreType.DMA
    grad = pl.pallas_call(
        kernel,
        out_shape=jax.ShapeDtypeStruct((ROWS, WIDTH), bf16),
        in_specs=[
            pl.BlockSpec(memory_space=pl.ANY),
            pl.BlockSpec(memory_space=pltpu.VMEM),
            pl.BlockSpec(memory_space=pl.ANY),
        ],
        out_specs=pl.BlockSpec(memory_space=pl.ANY),
        scratch_shapes=[
            pltpu.VMEM((2, 8, 2, 8, 16, WIDTH), bf16),
            pltpu.VMEM((ROWS, WIDTH), bf16),
            pltpu.VMEM((8, ROWS, 256), f32),
            pltpu.VMEM((ROWS, 2048), bf16),
            pltpu.VMEM((ROWS, 2048), bf16),
            pltpu.VMEM((ROWS, WIDTH), f32),
            pltpu.VMEM((ROWS, WIDTH), bf16),
            pltpu.VMEM((2, 2, 8, 128), f32),
            pltpu.VMEM((2, 8, 128), f32),
            pltpu.VMEM((4, 2, 8, 128), f32),
            pltpu.VMEM((X - 1, 2, 8, 128), f32),
            pltpu.VMEM((Y - 1, 2, 8, 128), f32),
            pltpu.VMEM((Z - 1, 2, 8, 128), f32),
            pltpu.VMEM((2, 2, 8, 128), f32),
            dma((10,)),
            dma((9,)), dma((9,)),
            dma((2, 2, 4, 3)), dma((2, 2, 4, 3)),
            dma((2, 2, 4, 4)), dma((2, 2, 4, 4)),
            dma((2, 5)), dma((2, 5)),
            dma((15,)), dma((15,)),
        ],
        compiler_params=pltpu.CompilerParams(
            collective_id=0, has_side_effects=True, vmem_limit_bytes=48 << 20
        ),
    )(activations.reshape(8, 16, WIDTH), token_ids, embed_table)
    return grad.reshape(1, 1, ROWS, WIDTH)


def solution(mesh):
    in_specs = (P("section", "dp", None), P(), P(("dp", "vocab"), None))
    out_specs = P(("dp", "vocab"), "section", None, None)
    return jax.shard_map(body, mesh=mesh, in_specs=in_specs, out_specs=out_specs, check_vma=False)
```

```python
import jax
import jax.numpy as jnp
from jax import lax
from jax.experimental import pallas as pl
from jax.experimental.pallas import tpu as pltpu
from jax.sharding import PartitionSpec as P

MESH = pl.DeviceIdType.MESH
COT, HID = 0, 1
Z, X, Y = 8, 4, 4
SLOTS = ((0, 1), (1, 2), (3, 2), (5, 2), (7, 1))
WIDTH = 2048
CUT_X, CUT_Y = 1024, 1664
COLUMNS = ((0, CUT_X), (CUT_X, CUT_Y - CUT_X), (CUT_Y, WIDTH - CUT_Y))
TILE = 512
ROWS = 256
DOT = dict(preferred_element_type=jnp.float32)


def merge(pairs):
    peak = pairs[0][0]
    for other, _ in pairs[1:]:
        peak = jnp.maximum(peak, other)
    total = pairs[0][1] * jnp.exp(pairs[0][0] - peak)
    for other, part in pairs[1:]:
        total = total + part * jnp.exp(other - peak)
    return peak, total


def kernel(
    act, ids_hbm, table, out,
    buf, ids, tab, scores, last_w, first_w, acc, out_v,
    own_stat, core_stat, sent_stat, plane_stat, z_stat, fin_stat,
    local_sem, boot_s, boot_r, z_s, z_r, ring_s, ring_r, core_s, core_r, stat_s, stat_r,
):
    s = lax.axis_index("section")
    d = lax.axis_index("dp")
    v = lax.axis_index("vocab")
    z, c = lax.div(d, 2), lax.rem(d, 2)
    yl, x = lax.div(v, 4), lax.rem(v, 4)
    y = 2 * s + yl
    row_first = (d * 8 + v) * 512 + s * ROWS

    def z_dev(k):
        return {"dp": lax.rem(z + k + Z, Z) * 2 + c}

    def x_dev(k):
        return {"vocab": yl * 4 + lax.rem(x + k + X, X)}

    def plane_dev(kx, ky):
        to = lax.rem(y + ky + Y, Y)
        over = lax.rem(x + kx + X, X)
        return {"section": lax.div(to, 2), "vocab": lax.rem(to, 2) * 4 + over}

    def y_dev(k):
        return plane_dev(0, k)

    core_dev = {"dp": z * 2 + 1 - c}
    cross_dev = {"section": 1 - s, "vocab": (1 - yl) * 4 + x}

    def remote(src, dst, send, recv, device):
        return pltpu.make_async_remote_copy(
            src_ref=src, dst_ref=dst, send_sem=send, recv_sem=recv,
            device_id=device, device_id_type=MESH,
        )

    load_own = pltpu.make_async_copy(act, buf.at[s, 0, c], local_sem.at[0])
    load_own.start()
    load_table = pltpu.make_async_copy(table.at[pl.ds(s * ROWS, ROWS)], tab, local_sem.at[1])
    load_table.start()
    load_ids = pltpu.make_async_copy(ids_hbm, ids, local_sem.at[2])
    load_ids.start()

    barrier = pltpu.get_barrier_semaphore()
    peers = [core_dev] + [dev(k) for dev in (x_dev, y_dev, z_dev) for k in (1, -1)]
    for peer in peers:
        pl.semaphore_signal(barrier, inc=1, device_id=peer, device_id_type=MESH)

    def region(array, slot, count, part, tile, tiles):
        first, width = COLUMNS[part]
        return buf.at[array, pl.ds(slot, count), c, pl.ds(tile, tiles), :, pl.ds(first, width)]

    def boot_copy(k):
        far_y = 3 - y
        if k == 0:
            ref = region(s, 0, 1, 0, 2 * x, 2)
        elif k == 1:
            ref = region(s, 0, 1, 1, 2 * far_y, 2)
        elif k == 2:
            ref = region(s, 0, 1, 2, 0, 8)
        elif k < 6:
            ref = region(s, 0, 1, 0, 2 * lax.rem(x + k - 2, X), 2)
        else:
            ref = region(s, 0, 1, 1, 2 * lax.rem(far_y + k - 5, Y), 2)
        return remote(ref, ref, boot_s.at[k], boot_r.at[k], cross_dev)

    def z_copy(array, way, t, part):
        slot = 0 if t == 0 else 2 * t - 1 + way
        to = 2 * t + 1 + way if t < 3 else 7
        quarter = 2 * (x, y, 0)[part]
        tiles = (2, 2, 8)[part]
        if t == 3:
            tiles = tiles // 2
            quarter = quarter + way * tiles
        return remote(
            region(array, slot, 1, part, quarter, tiles),
            region(array, to, 1, part, quarter, tiles),
            z_s.at[array, way, t, part], z_r.at[array, way, t, part],
            z_dev(1 if way == 0 else -1),
        )

    def ring_copy(array, dim, t, k):
        slot, count = SLOTS[t]
        q, dev = ((x, x_dev), (y, y_dev))[dim]
        if k < 2:
            tile, tiles = 2 * q, 2
        elif k == 2:
            tile, tiles = 2 * lax.rem(q + 3, 4), 1
        else:
            tile, tiles = 2 * lax.rem(q + 1, 4) + 1, 1
        ref = region(array, slot, count, dim, tile, tiles)
        return remote(
            ref, ref, ring_s.at[array, dim, t - 1, k], ring_r.at[array, dim, t - 1, k],
            dev(1 if k % 2 == 0 else -1),
        )

    def core_copy(array, t):
        slot, count = SLOTS[t]
        ref = buf.at[array, pl.ds(slot, count), c]
        return remote(ref, ref, core_s.at[array, t], core_r.at[array, t], core_dev)

    def start(array):
        for part in range(3):
            @pl.when(s != array)
            def _():
                boot_copy(part).wait_recv()

            for way in range(2):
                z_copy(array, way, 0, part).start()

    def step_quarters(array, t):
        for part in range(2):
            for way in range(2):
                z_copy(array, way, t - 1, part).wait_recv()
                if t < 4:
                    z_copy(array, way, t, part).start()
            for k in range(2):
                ring_copy(array, part, t, k).start()

    def step_whole(array, t):
        for way in range(2):
            z_copy(array, way, t - 1, 2).wait_recv()
            if t < 4:
                z_copy(array, way, t, 2).start()

    def pass_on(array, t):
        for dim in range(2):
            for k in range(2):
                ring_copy(array, dim, t, k).wait_recv()
                ring_copy(array, dim, t, k + 2).start()

    def share(array, t):
        for dim in range(2):
            for k in range(2):
                ring_copy(array, dim, t, k + 2).wait_recv()
        core_copy(array, t).start()

    def chip_of(slot):
        half = lax.div(slot + 1, 2)
        return lax.rem(z + jnp.where(lax.rem(slot, 2) == 1, Z - half, half), Z)

    def score(t):
        core_copy(HID, t).wait_recv()
        first, count = SLOTS[t]

        rows = buf[HID, pl.ds(first, count)].reshape(count * 256, WIDTH)
        block = lax.dot_general(tab[...], rows, (((1,), (1,)), ((), ())), **DOT)
        peak = jnp.max(block, axis=0, keepdims=True)
        total = jnp.sum(jnp.exp(block - peak), axis=0, keepdims=True)
        for k in range(count):
            scores[first + k] = block[:, k * 256 : k * 256 + 256]
            chip = chip_of(first + k)
            for core in range(2):
                lanes = slice(k * 256 + core * 128, k * 256 + core * 128 + 128)
                own_stat[core, 0, pl.ds(chip, 1), :] = peak[:, lanes]
                own_stat[core, 1, pl.ds(chip, 1), :] = total[:, lanes]

    def tile(n):
        return pl.ds(pl.multiple_of(n * TILE, TILE), TILE)

    def first_dot(first, count, cols):
        rows = buf[COT, pl.ds(first, count), :, :, :, cols].reshape(count * 256, TILE)
        return jnp.dot(first_w[:, first * 256 : (first + count) * 256], rows, **DOT)

    def add_first(t):
        first, count = SLOTS[t]
        core_copy(COT, t).wait_recv()

        def one(n, carry):
            cols = tile(n)
            part = first_dot(first, count, cols)
            acc[:, cols] = part if t == 0 else acc[:, cols] + part
            return carry

        lax.fori_loop(0, WIDTH // TILE, one, 0)

    def store(n):
        return pltpu.make_async_copy(
            out_v.at[:, tile(n)], out.at[:, tile(n)], local_sem.at[3 + n]
        )

    def hot(index, slot, core):
        at = pl.multiple_of(chip_of(slot) * 256 + core * 128, 128)
        wanted = ids[pl.ds(index, 1), pl.ds(at, 128)] - row_first
        return lax.broadcasted_iota(jnp.int32, (ROWS, 128), 0) == wanted

    def lanes_of(slot, core):
        return pl.ds(pl.multiple_of(slot * 256 + core * 128, 128), 128)

    def stat_core(k):
        if k == 0:
            return remote(own_stat.at[1 - c], core_stat, stat_s.at[0], stat_r.at[0], core_dev)
        return remote(sent_stat.at[3], fin_stat.at[c], stat_s.at[1], stat_r.at[1], core_dev)

    def stat_plane(k):
        dev = plane_dev(k % X, k // X)
        return remote(
            sent_stat.at[1], plane_stat.at[k - 1], stat_s.at[1 + k], stat_r.at[1 + k], dev
        )

    def stat_z(k):
        return remote(
            sent_stat.at[2], z_stat.at[k - 1], stat_s.at[16 + k], stat_r.at[16 + k], z_dev(k)
        )

    def stat_send(stage, pairs):
        peak, total = merge(pairs)
        sent_stat[stage, 0] = peak
        sent_stat[stage, 1] = total

    def stat_plane_send():
        stat_core(0).wait_recv()
        mine = own_stat[pl.ds(c, 1)]
        stat_send(1, [(mine[0, 0], mine[0, 1]), (core_stat[0], core_stat[1])])
        for k in range(1, X * Y):
            stat_plane(k).start()

    def stat_z_send():
        pairs = [(sent_stat[1, 0], sent_stat[1, 1])]
        for k in range(1, X * Y):
            stat_plane(k).wait_recv()
            pairs.append((plane_stat[k - 1, 0], plane_stat[k - 1, 1]))
        stat_send(2, pairs)
        for k in range(1, Z):
            stat_z(k).start()

    def stat_fin_send():
        pairs = [(sent_stat[2, 0], sent_stat[2, 1])]
        for k in range(1, Z):
            stat_z(k).wait_recv()
            pairs.append((z_stat[k - 1, 0], z_stat[k - 1, 1]))
        stat_send(3, pairs)
        stat_core(1).start()
        fin_stat[pl.ds(c, 1)] = sent_stat[pl.ds(3, 1)]

    def share_own(array):
        @pl.when(s != array)
        def _():
            for k in range(3, 9):
                boot_copy(k).wait_recv()
            core_copy(array, 0).start()

    load_own.wait()
    pl.semaphore_wait(barrier, len(peers))

    for k in range(3):
        boot_copy(k).start()
    start(HID)
    for k in range(3, 9):
        boot_copy(k).start()

    @pl.when(s == HID)
    def _():
        core_copy(HID, 0).start()

    @pl.when(s == COT)
    def _():
        core_copy(COT, 0).start()

    def first_rows(slot, carry):
        for core in range(2):
            first_w[:, lanes_of(slot, core)] = hot(0, slot, core).astype(jnp.bfloat16)
        return carry

    load_ids.wait()
    lax.fori_loop(0, 8, first_rows, 0)
    load_table.wait()

    step_quarters(HID, 1)
    step_whole(HID, 1)
    step_quarters(HID, 2)
    pass_on(HID, 1)
    step_whole(HID, 2)
    step_quarters(HID, 3)
    pass_on(HID, 2)
    step_whole(HID, 3)
    share_own(HID)
    share(HID, 1)
    start(COT)
    score(0)
    step_quarters(HID, 4)
    pass_on(HID, 3)
    step_whole(HID, 4)
    share(HID, 2)
    share_own(COT)
    score(1)
    pass_on(HID, 4)
    share(HID, 3)
    step_quarters(COT, 1)
    score(2)
    step_whole(COT, 1)
    share(HID, 4)
    score(3)
    score(4)
    stat_core(0).start()
    step_quarters(COT, 2)
    pass_on(COT, 1)
    stat_plane_send()
    step_whole(COT, 2)
    add_first(0)
    step_quarters(COT, 3)
    pass_on(COT, 2)
    share(COT, 1)
    stat_z_send()
    step_whole(COT, 3)
    step_quarters(COT, 4)
    pass_on(COT, 3)
    add_first(1)
    stat_fin_send()
    step_whole(COT, 4)
    share(COT, 2)
    pass_on(COT, 4)
    share(COT, 3)
    stat_core(1).wait_recv()

    def last_rows(slot, carry):
        chip = chip_of(slot)
        for core in range(2):
            peak = fin_stat[core, 0, pl.ds(chip, 1), :]
            total = fin_stat[core, 1, pl.ds(chip, 1), :]
            lanes = slice(core * 128, core * 128 + 128)
            probs = jnp.exp(scores[slot, :, lanes] - peak) / total
            weight = probs - jnp.where(hot(1, slot, core), 1.0, 0.0)
            last_w[:, lanes_of(slot, core)] = weight.astype(jnp.bfloat16)
        return carry

    lax.fori_loop(0, 8, last_rows, 0)

    add_first(2)

    def last_dot(n, carry):
        cols = tile(n)
        rows = buf[HID, :, :, :, :, cols].reshape(2048, TILE)
        acc[:, cols] = acc[:, cols] + jnp.dot(last_w[...], rows, **DOT)
        return carry

    lax.fori_loop(0, WIDTH // TILE, last_dot, 0)
    share(COT, 4)
    for t in range(3, 5):
        core_copy(COT, t).wait_recv()

    def finish(n, carry):
        cols = tile(n)
        total = acc[:, cols] + first_dot(5, 3, cols)
        out_v[:, cols] = total.astype(jnp.bfloat16)
        store(n).start()
        return carry

    lax.fori_loop(0, WIDTH // TILE, finish, 0)

    for k in range(9):
        boot_copy(k).wait_send()
    for array in range(2):
        for part in range(3):
            for way in range(2):
                for t in range(4):
                    z_copy(array, way, t, part).wait_send()
        for t in range(1, 5):
            for dim in range(2):
                for k in range(4):
                    ring_copy(array, dim, t, k).wait_send()
        for t in range(5):
            core_copy(array, t).wait_send()
    for k in range(2):
        stat_core(k).wait_send()
    for k in range(1, X * Y):
        stat_plane(k).wait_send()
    for k in range(1, Z):
        stat_z(k).wait_send()
    for n in range(WIDTH // TILE):
        store(n).wait()


def body(activations, token_ids, embed_table):
    bf16, f32, dma = jnp.bfloat16, jnp.float32, pltpu.SemaphoreType.DMA
    grad = pl.pallas_call(
        kernel,
        out_shape=jax.ShapeDtypeStruct((ROWS, WIDTH), bf16),
        in_specs=[
            pl.BlockSpec(memory_space=pltpu.HBM),
            pl.BlockSpec(memory_space=pltpu.HBM),
            pl.BlockSpec(memory_space=pltpu.HBM),
        ],
        out_specs=pl.BlockSpec(memory_space=pltpu.HBM),
        scratch_shapes=[
            pltpu.VMEM((2, 8, 2, 8, 16, WIDTH), bf16),
            pltpu.VMEM((2, 2048), jnp.int32),
            pltpu.VMEM((ROWS, WIDTH), bf16),
            pltpu.VMEM((8, ROWS, 256), f32),
            pltpu.VMEM((ROWS, 2048), bf16),
            pltpu.VMEM((ROWS, 2048), bf16),
            pltpu.VMEM((ROWS, WIDTH), f32),
            pltpu.VMEM((ROWS, WIDTH), bf16),
            pltpu.VMEM((2, 2, 8, 128), f32),
            pltpu.VMEM((2, 8, 128), f32),
            pltpu.VMEM((4, 2, 8, 128), f32),
            pltpu.VMEM((X * Y - 1, 2, 8, 128), f32),
            pltpu.VMEM((Z - 1, 2, 8, 128), f32),
            pltpu.VMEM((2, 2, 8, 128), f32),
            dma((3 + WIDTH // TILE,)),
            dma((9,)), dma((9,)),
            dma((2, 2, 4, 3)), dma((2, 2, 4, 3)),
            dma((2, 2, 4, 4)), dma((2, 2, 4, 4)),
            dma((2, 5)), dma((2, 5)),
            dma((24,)), dma((24,)),
        ],
        compiler_params=pltpu.CompilerParams(
            collective_id=0, has_side_effects=True, vmem_limit_bytes=67_043_328
        ),
    )(activations.reshape(8, 16, WIDTH), token_ids, embed_table)
    return grad.reshape(1, 1, ROWS, WIDTH)


def solution(mesh):
    in_specs = (P("section", "dp", None), P(), P(("dp", "vocab"), None))
    out_specs = P(("dp", "vocab"), "section", None, None)
    return jax.shard_map(body, mesh=mesh, in_specs=in_specs, out_specs=out_specs, check_vma=False)
```
